128 devices in a mesh: tm: 16 (over z, y), space: 8 (over x, core).
Axes of the slice: x: 4, y: 4, z: 4, core: 2. Of those that a mesh axis runs over, the one named last changes fastest.
Arguments:
- initial_guess: float32 [16, 1024, 1024], P('tm', 'space'), may hold values from -6 to 6
- start_field: float32 [1024, 1024], P('space'), may hold values from -6 to 6
- source_field: float32 [1024, 1024], P('space'), may hold values from -0.3 to 0.3
Outputs:
- final_states: float32 [16, 1024, 1024], P('tm', 'space')
The draws below stay inside these ranges and needn't reach their ends.
All inputs are finite; a program needn't handle non-finite values.
Results may differ from the reference program's by a relative error of at most 0.00013.
Values sent between devices are 32-bit elements; how exact they have to be, the bound alone decides.
No kernel may reach another device: no remote copies, remote signals or barrier semaphores. Data moves between devices by JAX's collectives and lax.ppermute only.
A program may use at most 64 MiB of HBM per device.

```python
import jax
import jax.numpy as jnp
from jax import lax

N = 1024
M = 16
ITERS = 1
K = 16


def levels(key, extent, split, smallest, high):
    factor_of = 1.0
    for position, shards_of in split:
        heights = jax.random.uniform(jax.random.fold_in(jax.random.fold_in(key, 6), position), (shards_of,), jnp.float32, smallest / len(split), high / len(split))
        factor_of = factor_of * jnp.repeat(jnp.exp(heights), extent[position] // shards_of).reshape((-1,) + (1,) * (len(extent) - 1 - position))
    return factor_of


def centred(own_key, shape, deviation, bound, shards=(), held_as=jnp.bfloat16):
    entries = deviation * jax.random.normal(own_key, shape, jnp.float32)
    if shards:
        entries = entries * levels(own_key, shape, shards, -0.22, 0.18)
    return jnp.clip(entries, -bound, bound).astype(held_as)


def setup_inputs(seed: int = 0) -> dict:
    arg_keys = jax.random.split(jax.random.key(seed), 4)
    return {
        "initial_guess": centred(arg_keys[0], (K, N, N), 1.0, 6.0, ((0, 16), (1, 8)), jnp.float32),
        "start_field": centred(arg_keys[1], (N, N), 1.0, 6.0, ((0, 8),), jnp.float32),
        "source_field": centred(arg_keys[2], (N, N), 0.05, 0.3, ((0, 8),), jnp.float32),
    }


decay_rate = 0.0005
spread_rate = 0.01


def mode_symbols():
    mode_index = jnp.arange(N).astype(jnp.float32)
    half_sines = jnp.sin(jnp.pi * mode_index / N) ** 2
    stiffness = 4.0 * (half_sines[:, None] + half_sines[None, :])
    fine_factor = 1.0 / (1.0 + decay_rate + spread_rate * stiffness)
    coarse_factor = 1.0 / (1.0 + M * decay_rate + M * spread_rate * stiffness)
    fine_power = jnp.ones_like(fine_factor)
    forcing_symbol = jnp.zeros_like(fine_factor)
    for substep in range(M):
        fine_power = fine_power * fine_factor
        forcing_symbol = forcing_symbol + fine_power
    return fine_power, forcing_symbol, coarse_factor


def propagate(symbol, fields):
    return jnp.real(jnp.fft.ifft2(symbol * jnp.fft.fft2(fields))).astype(jnp.float32)


def reference(initial_guess, start_field, source_field):
    fine_power, forcing_symbol, coarse_factor = mode_symbols()
    forcing = propagate(forcing_symbol, source_field)
    states = initial_guess
    for iteration in range(ITERS):
        previous = jnp.concatenate([start_field[None], states[:-1]], axis=0)
        relaxed = propagate(fine_power, previous) + forcing
        previous_relaxed = jnp.concatenate([start_field[None], relaxed[:-1]], axis=0)
        residual = propagate(fine_power, previous_relaxed) + forcing - relaxed
        residual_hat = jnp.fft.fft2(residual)

        def advance(carried, current):
            updated = coarse_factor * carried + current
            return updated, updated

        unused, errors_hat = lax.scan(advance, jnp.zeros_like(residual_hat[0]), residual_hat)
        states = relaxed + jnp.real(jnp.fft.ifft2(errors_hat)).astype(jnp.float32)
    return states
```

```python
import functools

import jax
import jax.numpy as jnp
import ml_dtypes
import numpy as np
from jax import lax
from jax.experimental import pallas as pl
from jax.experimental.pallas import tpu as pltpu
from jax.sharding import PartitionSpec as P

M = 16
RADIX = 8
RESIDUES = (0, 4, 1, 7, 2, 6, 3, 5)
AXES = ("tm", "space")

decay_rate = 0.0005
spread_rate = 0.01


def kernel_matrices(length):
    width = length // RADIX
    cells = np.arange(width)

    def cas(modes, sign):
        angles = 2.0 * np.pi / length * (cells[:, None] * modes[None, :] % length)
        return np.cos(angles) + sign * np.sin(angles)

    def modes(residue):
        return residue + RADIX * np.arange(width)

    zero = np.zeros((width, width))
    matrices = [np.block([[cas(modes(0), 1), zero], [zero, cas(modes(4), 1)]])]
    for q in (1, 2, 3):
        one, other = modes(q), modes(RADIX - q)
        matrices.append(np.block([[cas(one, 1), cas(other, 1)], [cas(one, -1), -cas(other, -1)]]))
    full = np.stack(matrices).astype(np.float32)
    high = full.astype(ml_dtypes.bfloat16)
    low = (full - high.astype(np.float32)).astype(ml_dtypes.bfloat16)
    return high, low


def product(value, high, low, contract):
    value_high = value.astype(jnp.bfloat16)
    value_low = (value - value_high.astype(jnp.float32)).astype(jnp.bfloat16)
    dims = (((1,), (contract,)), ((), ()))
    dot = functools.partial(lax.dot_general, dimension_numbers=dims, preferred_element_type=jnp.float32)
    return dot(value_high, high) + (dot(value_low, high) + dot(value_high, low))


def to_modes(v, high, low):
    root = float(np.sqrt(0.5))
    s = [v[b] + v[b + 4] for b in range(4)]
    d = [v[b] - v[b + 4] for b in range(4)]
    even, odd = s[0] + s[2], s[1] + s[3]
    near, far = root * (d[1] - d[3]), root * (d[1] + d[3])
    pairs = (
        (even + odd, even - odd),
        (d[0] + near, far + d[2]),
        (s[0] - s[2], s[1] - s[3]),
        (d[0] - near, far - d[2]),
    )
    return [product(jnp.concatenate(pair, axis=1), high[i], low[i], 0) for i, pair in enumerate(pairs)]


def to_cells(h, high, low):
    root = float(np.sqrt(0.5))
    width = h[0].shape[1] // 2
    pairs = [product(h[i], high[i], low[i], 1) for i in range(4)]
    (a0, a4), (a1, b1), (a2, b2), (a3, b3) = [(pair[:, :width], pair[:, width:]) for pair in pairs]
    e, g = a0 + a4, a0 - a4
    p, m, q, n = a1 + a3, a1 - a3, b1 + b3, b1 - b3
    ep, em, gp, gm = e + a2, e - a2, g + b2, g - b2
    up, down = root * (m + q), root * (q - m)
    return [ep + p, gp + up, em + n, gm + down, ep - p, gp - up, em - n, gm - down]


def columns_forward(guess_ref, start_ref, source_ref, high_ref, low_ref, out_ref, field, copied):
    last = lax.axis_size("tm") - 1
    place = lax.axis_index("tm")

    def fetch(ref):
        copy = pltpu.make_async_copy(ref, field, copied)
        copy.start()
        copy.wait()

    @pl.when(place < last - 1)
    def _():
        fetch(guess_ref.at[0])

    @pl.when(place == last - 1)
    def _():
        fetch(start_ref)

    @pl.when(place == last)
    def _():
        fetch(source_ref)

    width = field.shape[1] // RADIX
    v = [field[:, b * width : (b + 1) * width] for b in range(RADIX)]
    h = to_modes(v, high_ref, low_ref)
    for i in range(4):
        out_ref[2 * width * i : 2 * width * (i + 1), :] = h[i].T


def rows_and_time(in_ref, high_ref, low_ref, out_ref):
    times, blocks, group, width = in_ref.shape
    length = blocks * width
    rows = times * group
    v = [in_ref[:, b].reshape(rows, width) for b in range(blocks)]
    h = to_modes(v, high_ref, low_ref)

    device = lax.axis_index("tm") * lax.axis_size("space") + lax.axis_index("space")
    groups = width // group
    residue = jnp.int32(0)
    for i, q in enumerate(RESIDUES):
        residue = jnp.where(device // groups == i, q, residue)
    within = lax.rem(device, groups) * group
    sublane = lax.broadcasted_iota(jnp.int32, (group, 2 * width), 0)
    lane = lax.broadcasted_iota(jnp.int32, (group, 2 * width), 1)
    column_modes = residue + RADIX * (within + sublane)

    def half_sines(modes):
        return jnp.sin(jnp.pi / length * modes.astype(jnp.float32)) ** 2

    column_sines = half_sines(column_modes)
    outs = []
    for i in range(4):
        first, second = RESIDUES[2 * i], RESIDUES[2 * i + 1]
        row_modes = jnp.where(lane < width, first + RADIX * lane, second + RADIX * (lane - width))
        stiffness = 4.0 * (half_sines(row_modes) + column_sines)
        fine = 1.0 / (1.0 + decay_rate + spread_rate * stiffness)
        coarse = 1.0 / (1.0 + M * decay_rate + M * spread_rate * stiffness)
        power, forcing_symbol = fine, fine
        for _ in range(M - 1):
            power = power * fine
            forcing_symbol = forcing_symbol + power
        scale = 1.0 / (length * length)
        scaled_power = scale * power
        part = [h[i][t * group : (t + 1) * group] for t in range(times)]
        forcing = scale * forcing_symbol * part[times - 1]
        relaxed = scaled_power * part[times - 2] + forcing
        state = relaxed
        states = [state]
        gap = power - coarse
        for j in range(1, times):
            state = coarse * state + (gap * relaxed + forcing)
            states.append(state)
            if j < times - 1:
                relaxed = scaled_power * part[j - 1] + forcing
        outs.append(jnp.concatenate(states, axis=0))

    cells = to_cells(outs, high_ref, low_ref)
    for b in range(blocks):
        out_ref[:, b] = cells[b].reshape(times, group, width)


def columns_inverse(in_ref, high_ref, low_ref, out_ref):
    width = in_ref.shape[1]
    h = [in_ref[2 * width * i : 2 * width * (i + 1), :].T for i in range(4)]
    cells = to_cells(h, high_ref, low_ref)
    for b in range(RADIX):
        out_ref[0, :, b * width : (b + 1) * width] = cells[b]


def on_chip(count):
    return [pl.BlockSpec(memory_space=pltpu.VMEM)] * count


def anywhere(count):
    return [pl.BlockSpec(memory_space=pl.ANY)] * count


def body(initial_guess, start_field, source_field):
    rows, length = start_field.shape
    times, blocks = lax.axis_size("tm"), lax.axis_size("space")
    devices = times * blocks
    group = length // devices
    high, low = (jnp.asarray(part) for part in kernel_matrices(length))

    spectra = pl.pallas_call(
        columns_forward,
        out_shape=jax.ShapeDtypeStruct((length, rows), jnp.float32),
        in_specs=anywhere(3) + on_chip(2),
        out_specs=on_chip(1)[0],
        scratch_shapes=[pltpu.VMEM((rows, length), jnp.float32), pltpu.SemaphoreType.DMA],
        name="columns_forward",
    )(initial_guess, start_field, source_field, high, low)

    spectra = spectra.reshape(devices, group, rows)
    spectra = lax.all_to_all(spectra, AXES, split_axis=0, concat_axis=0, tiled=True)
    states = pl.pallas_call(
        rows_and_time,
        out_shape=jax.ShapeDtypeStruct((times, blocks, group, rows), jnp.float32),
        in_specs=on_chip(3),
        out_specs=on_chip(1)[0],
        name="rows_and_time",
    )(spectra.reshape(times, blocks, group, rows), high, low)

    states = states.reshape(devices, group, rows)
    states = lax.all_to_all(states, AXES, split_axis=0, concat_axis=0, tiled=True)
    return pl.pallas_call(
        columns_inverse,
        out_shape=jax.ShapeDtypeStruct((1, rows, length), jnp.float32),
        in_specs=on_chip(3),
        out_specs=on_chip(1)[0],
        name="columns_inverse",
    )(states.reshape(length, rows), high, low)


def solution(mesh):
    in_specs = (P("tm", "space", None), P("space", None), P("space", None))
    out_specs = P("tm", "space", None)
    return jax.shard_map(body, mesh=mesh, in_specs=in_specs, out_specs=out_specs, check_vma=False)
```

```python
import functools

import jax
import jax.numpy as jnp
import ml_dtypes
import numpy as np
from jax import lax
from jax.experimental import pallas as pl
from jax.experimental.pallas import tpu as pltpu
from jax.sharding import Mesh
from jax.sharding import PartitionSpec as P

M = 16
RADIX = 8
RESIDUES = (0, 4, 1, 1, 2, 2, 3, 3)
AXES = ("core", "z", "y", "x")
TM, SPACE = ("z", "y"), ("x", "core")
LIMIT = pltpu.CompilerParams(vmem_limit_bytes=8 * 1024 * 1024)

decay_rate = 0.0005
spread_rate = 0.01


def kernel_matrices(length):
    width = length // RADIX
    cells = np.arange(width)

    def cas(residue, sign):
        modes = residue + RADIX * np.arange(width)
        angles = 2.0 * np.pi / length * (cells[:, None] * modes[None, :] % length)
        return np.cos(angles) + sign * np.sin(angles)

    blocks = [cas(0, 1), cas(4, 1)] + [cas(q, sign) for q in (1, 2, 3) for sign in (1, -1)]
    full = np.stack(blocks).astype(np.float32)
    high = full.astype(ml_dtypes.bfloat16)
    low = (full - high.astype(np.float32)).astype(ml_dtypes.bfloat16)
    return high, low


def matrix(blocks, i):
    one, other = blocks[2 * i], blocks[2 * i + 1]
    if i == 0:
        zero = jnp.zeros_like(one)
        rows = ((one, zero), (zero, other))
    else:
        rows = ((one, other), (other, -one))
    return jnp.concatenate([jnp.concatenate(row, axis=1) for row in rows], axis=0)


def product(value, high, low, i, contract):
    value_high = value.astype(jnp.bfloat16)
    value_low = (value - value_high.astype(jnp.float32)).astype(jnp.bfloat16)
    dims = (((1,), (contract,)), ((), ()))
    dot = functools.partial(lax.dot_general, dimension_numbers=dims, preferred_element_type=jnp.float32)
    matrix_high, matrix_low = matrix(high, i), matrix(low, i)
    return dot(value_high, matrix_high) + (dot(value_low, matrix_high) + dot(value_high, matrix_low))


def to_pairs(v):
    root = float(np.sqrt(0.5))
    s = [v[b] + v[b + 4] for b in range(4)]
    d = [v[b] - v[b + 4] for b in range(4)]
    even, odd = s[0] + s[2], s[1] + s[3]
    near, far = root * (d[1] - d[3]), root * (d[1] + d[3])
    pairs = (
        (even + odd, even - odd),
        (d[0] + near, far + d[2]),
        (s[0] - s[2], s[1] - s[3]),
        (d[0] - near, far - d[2]),
    )
    return [jnp.concatenate(pair, axis=1) for pair in pairs]


def to_modes(pairs, high, low):
    return [product(pair, high, low, i, 0) for i, pair in enumerate(pairs)]


def to_cells(h, high, low):
    root = float(np.sqrt(0.5))
    width = h[0].shape[1] // 2
    pairs = [product(h[i], high, low, i, 1) for i in range(4)]
    (a0, a4), (a1, b1), (a2, b2), (a3, b3) = [(pair[:, :width], pair[:, width:]) for pair in pairs]
    e, g = a0 + a4, a0 - a4
    p, m, q, n = a1 + a3, a1 - a3, b1 + b3, b1 - b3
    ep, em, gp, gm = e + a2, e - a2, g + b2, g - b2
    up, down = root * (m + q), root * (q - m)
    return [ep + p, gp + up, em + n, gm + down, ep - p, gp - up, em - n, gm - down]


def columns_forward(guess_ref, start_ref, source_ref, high_ref, low_ref, out_ref, field, high, low, copied):
    last = lax.axis_size("z") * lax.axis_size("y") - 1
    place = lax.axis_index("z") * lax.axis_size("y") + lax.axis_index("y")

    def fetch(ref):
        pltpu.make_async_copy(ref, field, copied.at[0]).start()

    @pl.when(place < last - 1)
    def _():
        fetch(guess_ref.at[0])

    @pl.when(place == last - 1)
    def _():
        fetch(start_ref)

    @pl.when(place == last)
    def _():
        fetch(source_ref)

    matrices = [
        pltpu.make_async_copy(high_ref, high, copied.at[1]),
        pltpu.make_async_copy(low_ref, low, copied.at[2]),
    ]
    for copy in matrices:
        copy.start()
    pltpu.make_async_copy(start_ref, field, copied.at[0]).wait()

    width = field.shape[1] // RADIX
    pairs = to_pairs([field[:, b * width : (b + 1) * width] for b in range(RADIX)])
    for copy in matrices:
        copy.wait()
    h = to_modes(pairs, high, low)
    for i in range(4):
        out_ref[2 * width * i : 2 * width * (i + 1), :] = h[i].T


def rows_and_time(in_ref, high_ref, low_ref, out_ref):
    cores, times, chips, group, width = in_ref.shape
    length = chips * cores * width
    rows = times * group
    v = [in_ref[b % cores, :, b // cores].reshape(rows, width) for b in range(chips * cores)]
    h = to_modes(to_pairs(v), high_ref, low_ref)

    device = 0
    for axis in AXES:
        device = device * lax.axis_size(axis) + lax.axis_index(axis)
    groups = width // group
    residue = jnp.int32(0)
    for i, q in enumerate(RESIDUES):
        residue = jnp.where(device // groups == i, q, residue)
    within = lax.rem(device, groups) * group
    sublane = lax.broadcasted_iota(jnp.int32, (group, width), 0)
    lane = lax.broadcasted_iota(jnp.int32, (group, width), 1)

    def half_sines(modes):
        return jnp.sin(jnp.pi / length * modes.astype(jnp.float32)) ** 2

    column_sines = half_sines(residue + RADIX * (within + sublane))

    def symbols(row_residue):
        stiffness = 4.0 * (half_sines(row_residue + RADIX * lane) + column_sines)
        fine = 1.0 / (1.0 + decay_rate + spread_rate * stiffness)
        coarse = 1.0 / (1.0 + M * decay_rate + M * spread_rate * stiffness)
        power, forcing_symbol = fine, fine
        for _ in range(M - 1):
            power = power * fine
            forcing_symbol = forcing_symbol + power
        return power, forcing_symbol, coarse

    known = {q: symbols(q) for q in sorted(set(RESIDUES))}
    outs = []
    for i in range(4):
        both = zip(known[RESIDUES[2 * i]], known[RESIDUES[2 * i + 1]])
        power, forcing_symbol, coarse = (jnp.concatenate(pair, axis=1) for pair in both)
        scale = 1.0 / (length * length)
        scaled_power = scale * power
        part = [h[i][t * group : (t + 1) * group] for t in range(times)]
        forcing = scale * forcing_symbol * part[times - 1]
        relaxed = scaled_power * part[times - 2] + forcing
        state = relaxed
        states = [state]
        gap = power - coarse
        for j in range(1, times):
            state = coarse * state + (gap * relaxed + forcing)
            states.append(state)
            if j < times - 1:
                relaxed = scaled_power * part[j - 1] + forcing
        outs.append(jnp.concatenate(states, axis=0))

    cells = to_cells(outs, high_ref, low_ref)
    for b in range(chips * cores):
        out_ref[b % cores, :, b // cores] = cells[b].reshape(times, group, width)


def columns_inverse(in_ref, high_ref, low_ref, out_ref):
    width = in_ref.shape[1]
    h = [in_ref[2 * width * i : 2 * width * (i + 1), :].T for i in range(4)]
    cells = to_cells(h, high_ref, low_ref)
    for b in range(RADIX):
        out_ref[0, :, b * width : (b + 1) * width] = cells[b]


def on_chip(count):
    return [pl.BlockSpec(memory_space=pltpu.VMEM)] * count


def off_chip(count):
    return [pl.BlockSpec(memory_space=pltpu.HBM)] * count


def body(initial_guess, start_field, source_field):
    rows, length = start_field.shape
    times, chips, cores = lax.axis_size(TM), lax.axis_size("x"), lax.axis_size("core")
    devices = times * chips * cores
    group = length // devices
    high, low = (jnp.asarray(part) for part in kernel_matrices(length))

    spectra = pl.pallas_call(
        columns_forward,
        out_shape=jax.ShapeDtypeStruct((length, rows), jnp.float32),
        in_specs=off_chip(5),
        out_specs=on_chip(1)[0],
        scratch_shapes=[
            pltpu.VMEM((rows, length), jnp.float32),
            pltpu.VMEM(high.shape, high.dtype),
            pltpu.VMEM(low.shape, low.dtype),
            pltpu.SemaphoreType.DMA((3,)),
        ],
        compiler_params=LIMIT,
        name="columns_forward",
    )(*(pltpu.with_memory_space_constraint(x, pltpu.HBM) for x in (initial_guess, start_field, source_field, high, low)))

    spectra = spectra.reshape(devices, group, rows)
    spectra = lax.all_to_all(spectra, AXES, split_axis=0, concat_axis=0, tiled=True)
    states = pl.pallas_call(
        rows_and_time,
        out_shape=jax.ShapeDtypeStruct((cores, times, chips, group, rows), jnp.float32),
        in_specs=on_chip(3),
        out_specs=on_chip(1)[0],
        compiler_params=LIMIT,
        name="rows_and_time",
    )(spectra.reshape(cores, times, chips, group, rows), high, low)

    states = states.reshape(devices, group, rows)
    states = lax.all_to_all(states, AXES, split_axis=0, concat_axis=0, tiled=True)
    return pl.pallas_call(
        columns_inverse,
        out_shape=jax.ShapeDtypeStruct((1, rows, length), jnp.float32),
        in_specs=on_chip(3),
        out_specs=on_chip(1)[0],
        compiler_params=LIMIT,
        name="columns_inverse",
    )(states.reshape(length, rows), high, low)


def solution(mesh):
    chips = mesh.shape["space"] // 2
    finer = Mesh(mesh.devices.reshape(4, -1, chips, 2), TM + SPACE)
    in_specs = (P(TM, SPACE, None), P(SPACE, None), P(SPACE, None))
    out_specs = P(TM, SPACE, None)
    return jax.shard_map(body, mesh=finer, in_specs=in_specs, out_specs=out_specs, check_vma=False)
```

```python
import jax
import jax.numpy as jnp
import ml_dtypes
import numpy as np
from jax import lax
from jax.experimental import pallas as pl
from jax.experimental.pallas import tpu as pltpu
from jax.sharding import Mesh
from jax.sharding import PartitionSpec as P

M = 16
RADIX = 8
RESIDUES = (0, 4, 1, 1, 2, 2, 3, 3)
AXES = ("core", "z", "x", "y")
TM, SPACE = ("z", "y"), ("x", "core")
LIMIT = pltpu.CompilerParams(vmem_limit_bytes=8 * 1024 * 1024)

decay_rate = 0.0005
spread_rate = 0.01


def kernel_matrices(length):
    width = length // RADIX
    cells = np.arange(width)

    def cas(residue, sign):
        modes = residue + RADIX * np.arange(width)
        angles = 2.0 * np.pi / length * (cells[:, None] * modes[None, :] % length)
        return np.cos(angles) + sign * np.sin(angles)

    blocks = [cas(0, 1), cas(4, 1)] + [cas(q, sign) for q in (1, 2, 3) for sign in (1, -1)]
    full = np.stack(blocks).astype(np.float32)
    high = full.astype(ml_dtypes.bfloat16)
    low = (full - high.astype(np.float32)).astype(ml_dtypes.bfloat16)
    return high, low


def matrix(blocks, i):
    one, other = blocks[2 * i], blocks[2 * i + 1]
    if i == 0:
        zero = jnp.zeros_like(one)
        rows = ((one, zero), (zero, other))
    else:
        rows = ((one, other), (other, -one))
    return jnp.concatenate([jnp.concatenate(row, axis=1) for row in rows], axis=0)


def split(value):
    high = value.astype(jnp.bfloat16)
    low = (value - high.astype(jnp.float32)).astype(jnp.bfloat16)
    return jnp.concatenate([high, low], axis=0)


def product(value, high, low, i):
    count = value.shape[0]
    parts = split(value)
    twice = jnp.dot(parts, matrix(high, i), preferred_element_type=jnp.float32)
    once = jnp.dot(parts[:count], matrix(low, i), preferred_element_type=jnp.float32)
    return twice[:count] + (twice[count:] + once)


def product_across(value, high, low, i):
    count, modes = value.shape
    matrices = jnp.concatenate([matrix(high, i), matrix(low, i)], axis=0)
    dims = (((1,), (1,)), ((), ()))
    both = lax.dot_general(matrices, split(value), dims, preferred_element_type=jnp.float32)
    return both[:modes, :count] + (both[:modes, count:] + both[modes:, :count])


def to_pairs(v):
    root = float(np.sqrt(0.5))
    s = [v[b] + v[b + 4] for b in range(4)]
    d = [v[b] - v[b + 4] for b in range(4)]
    even, odd = s[0] + s[2], s[1] + s[3]
    near, far = root * (d[1] - d[3]), root * (d[1] + d[3])
    pairs = (
        (even + odd, even - odd),
        (d[0] + near, far + d[2]),
        (s[0] - s[2], s[1] - s[3]),
        (d[0] - near, far - d[2]),
    )
    return [jnp.concatenate(pair, axis=1) for pair in pairs]


def to_modes(pairs, high, low):
    return [product(pair, high, low, i) for i, pair in enumerate(pairs)]


def to_cells(h, high, low):
    root = float(np.sqrt(0.5))
    width = h[0].shape[1] // 2
    pairs = [product(h[i], high, low, i) for i in range(4)]
    (a0, a4), (a1, b1), (a2, b2), (a3, b3) = [(pair[:, :width], pair[:, width:]) for pair in pairs]
    e, g = a0 + a4, a0 - a4
    p, m, q, n = a1 + a3, a1 - a3, b1 + b3, b1 - b3
    ep, em, gp, gm = e + a2, e - a2, g + b2, g - b2
    up, down = root * (m + q), root * (q - m)
    return [ep + p, gp + up, em + n, gm + down, ep - p, gp - up, em - n, gm - down]


def columns_forward(guess_ref, start_ref, source_ref, high_ref, low_ref, out_ref, field, high, low, copied):
    last = lax.axis_size("z") * lax.axis_size("y") - 1
    place = lax.axis_index("z") * lax.axis_size("y") + lax.axis_index("y")

    def fetch(ref):
        pltpu.make_async_copy(ref, field, copied.at[0]).start()

    @pl.when(place < last - 1)
    def _():
        fetch(guess_ref.at[0])

    @pl.when(place == last - 1)
    def _():
        fetch(start_ref)

    @pl.when(place == last)
    def _():
        fetch(source_ref)

    matrices = [
        pltpu.make_async_copy(high_ref, high, copied.at[1]),
        pltpu.make_async_copy(low_ref, low, copied.at[2]),
    ]
    for copy in matrices:
        copy.start()
    pltpu.make_async_copy(start_ref, field, copied.at[0]).wait()

    width = field.shape[1] // RADIX
    pairs = to_pairs([field[:, b * width : (b + 1) * width] for b in range(RADIX)])
    for copy in matrices:
        copy.wait()
    for i in range(4):
        out_ref[2 * width * i : 2 * width * (i + 1), :] = product_across(pairs[i], high, low, i)


def rows_and_time(in_ref, high_ref, low_ref, high_across_ref, low_across_ref, out_ref):
    group, width = in_ref.shape[len(AXES) :]
    sizes = dict(zip(AXES, in_ref.shape))
    times, blocks = sizes["z"] * sizes["y"], sizes["x"] * sizes["core"]
    length = blocks * width
    rows = times * group

    def of_block(b):
        place = {"x": b // sizes["core"], "core": b % sizes["core"]}
        return tuple(place.get(axis, slice(None)) for axis in AXES)

    v = [in_ref[of_block(b)].reshape(rows, width) for b in range(blocks)]
    h = to_modes(to_pairs(v), high_ref, low_ref)

    device = 0
    for axis in AXES:
        device = device * lax.axis_size(axis) + lax.axis_index(axis)
    groups = width // group
    residue = jnp.int32(0)
    for i, q in enumerate(RESIDUES):
        residue = jnp.where(device // groups == i, q, residue)
    within = lax.rem(device, groups) * group
    sublane = lax.broadcasted_iota(jnp.int32, (group, width), 0)
    lane = lax.broadcasted_iota(jnp.int32, (group, width), 1)

    def half_sines(modes):
        return jnp.sin(jnp.pi / length * modes.astype(jnp.float32)) ** 2

    column_sines = half_sines(residue + RADIX * (within + sublane))

    def symbols(row_residue):
        stiffness = 4.0 * (half_sines(row_residue + RADIX * lane) + column_sines)
        fine = 1.0 / (1.0 + decay_rate + spread_rate * stiffness)
        coarse = 1.0 / (1.0 + M * decay_rate + M * spread_rate * stiffness)
        power, forcing_symbol = fine, fine
        for _ in range(M - 1):
            power = power * fine
            forcing_symbol = forcing_symbol + power
        return power, forcing_symbol, coarse

    known = {q: symbols(q) for q in sorted(set(RESIDUES))}
    outs = []
    for i in range(4):
        both = zip(known[RESIDUES[2 * i]], known[RESIDUES[2 * i + 1]])
        power, forcing_symbol, coarse = (jnp.concatenate(pair, axis=1) for pair in both)
        scale = 1.0 / (length * length)
        scaled_power = scale * power
        part = [h[i][t * group : (t + 1) * group] for t in range(times)]
        forcing = scale * forcing_symbol * part[times - 1]
        relaxed = scaled_power * part[times - 2] + forcing
        state = relaxed
        states = [state]
        gap = power - coarse
        for j in range(1, times):
            state = coarse * state + (gap * relaxed + forcing)
            states.append(state)
            if j < times - 1:
                relaxed = scaled_power * part[j - 1] + forcing
        outs.append(jnp.concatenate(states, axis=0))

    cells = to_cells(outs, high_across_ref, low_across_ref)
    for b in range(blocks):
        place = of_block(b)
        out_ref[place] = cells[b].reshape(sizes["z"], sizes["y"], group, width)


def columns_inverse(in_ref, high_ref, low_ref, out_ref):
    width = in_ref.shape[1]
    h = [in_ref[2 * width * i : 2 * width * (i + 1), :].T for i in range(4)]
    cells = to_cells(h, high_ref, low_ref)
    for b in range(RADIX):
        out_ref[0, :, b * width : (b + 1) * width] = cells[b]


def on_chip(count):
    return [pl.BlockSpec(memory_space=pltpu.VMEM)] * count


def off_chip(count):
    return [pl.BlockSpec(memory_space=pltpu.HBM)] * count


def body(initial_guess, start_field, source_field):
    rows, length = start_field.shape
    devices = lax.axis_size(AXES)
    tiles = tuple(lax.axis_size(axis) for axis in AXES)
    group = length // devices
    matrices = kernel_matrices(length)
    high, low = (jnp.asarray(part) for part in matrices)
    high_across, low_across = (jnp.asarray(np.swapaxes(part, 1, 2)) for part in matrices)

    spectra = pl.pallas_call(
        columns_forward,
        out_shape=jax.ShapeDtypeStruct((length, rows), jnp.float32),
        in_specs=off_chip(5),
        out_specs=on_chip(1)[0],
        scratch_shapes=[
            pltpu.VMEM((rows, length), jnp.float32),
            pltpu.VMEM(high.shape, high.dtype),
            pltpu.VMEM(low.shape, low.dtype),
            pltpu.SemaphoreType.DMA((3,)),
        ],
        compiler_params=LIMIT,
        name="columns_forward",
    )(*(pltpu.with_memory_space_constraint(x, pltpu.HBM) for x in (initial_guess, start_field, source_field, high_across, low_across)))

    spectra = spectra.reshape(devices, group, rows)
    spectra = lax.all_to_all(spectra, AXES, split_axis=0, concat_axis=0, tiled=True)
    states = pl.pallas_call(
        rows_and_time,
        out_shape=jax.ShapeDtypeStruct(tiles + (group, rows), jnp.float32),
        in_specs=on_chip(5),
        out_specs=on_chip(1)[0],
        compiler_params=LIMIT,
        name="rows_and_time",
    )(spectra.reshape(tiles + (group, rows)), high, low, high_across, low_across)

    states = states.reshape(devices, group, rows)
    states = lax.all_to_all(states, AXES, split_axis=0, concat_axis=0, tiled=True)
    return pl.pallas_call(
        columns_inverse,
        out_shape=jax.ShapeDtypeStruct((1, rows, length), jnp.float32),
        in_specs=on_chip(3),
        out_specs=on_chip(1)[0],
        compiler_params=LIMIT,
        name="columns_inverse",
    )(states.reshape(length, rows), high_across, low_across)


def solution(mesh):
    chips = mesh.shape["space"] // 2
    finer = Mesh(mesh.devices.reshape(4, -1, chips, 2), TM + SPACE)
    in_specs = (P(TM, SPACE, None), P(SPACE, None), P(SPACE, None))
    out_specs = P(TM, SPACE, None)
    return jax.shard_map(body, mesh=finer, in_specs=in_specs, out_specs=out_specs, check_vma=False)
```

```python
import jax
import jax.numpy as jnp
import ml_dtypes
import numpy as np
from jax import lax
from jax.experimental import pallas as pl
from jax.experimental.pallas import tpu as pltpu
from jax.sharding import Mesh
from jax.sharding import PartitionSpec as P

M = 16
RADIX = 8
RESIDUES = (0, 4, 1, 1, 2, 2, 3, 3)
AXES = ("core", "z", "x", "y")
TM, SPACE = ("z", "y"), ("x", "core")
LIMIT = pltpu.CompilerParams(vmem_limit_bytes=8 * 1024 * 1024)

decay_rate = 0.0005
spread_rate = 0.01


def kernel_matrices(length):
    width = length // RADIX
    cells = np.arange(width)

    def cas(residue, sign):
        modes = residue + RADIX * np.arange(width)
        angles = 2.0 * np.pi / length * (cells[:, None] * modes[None, :] % length)
        return np.cos(angles) + sign * np.sin(angles)

    blocks = [cas(0, 1), cas(4, 1)] + [cas(q, sign) for q in (1, 2, 3) for sign in (1, -1)]
    full = np.stack(blocks).astype(np.float32)
    high = full.astype(ml_dtypes.bfloat16)
    low = (full - high.astype(np.float32)).astype(ml_dtypes.bfloat16)
    return high, low


def matrix(blocks, i):
    one, other = blocks[2 * i], blocks[2 * i + 1]
    if i == 0:
        zero = jnp.zeros_like(one)
        rows = ((one, zero), (zero, other))
    else:
        rows = ((one, other), (other, -one))
    return jnp.concatenate([jnp.concatenate(row, axis=1) for row in rows], axis=0)


def split(value):
    high = value.astype(jnp.bfloat16)
    low = (value - high.astype(jnp.float32)).astype(jnp.bfloat16)
    return jnp.concatenate([high, low], axis=0)


def product(value, high, low, i):
    count = value.shape[0]
    parts = split(value)
    twice = jnp.dot(parts, matrix(high, i), preferred_element_type=jnp.float32)
    once = jnp.dot(parts[:count], matrix(low, i), preferred_element_type=jnp.float32)
    return twice[:count] + (twice[count:] + once)


def product_across(value, high, low, i):
    count, modes = value.shape
    matrices = jnp.concatenate([matrix(high, i), matrix(low, i)], axis=0)
    dims = (((1,), (1,)), ((), ()))
    both = lax.dot_general(matrices, split(value), dims, preferred_element_type=jnp.float32)
    return both[:modes, :count] + (both[:modes, count:] + both[modes:, :count])


def product_down(value, high, low, i):
    count = value.shape[1]
    top = value.astype(jnp.bfloat16)
    rest = (value - top.astype(jnp.float32)).astype(jnp.bfloat16)
    parts = jnp.concatenate([top, rest], axis=1)
    dims = (((0,), (0,)), ((), ()))
    twice = lax.dot_general(parts, matrix(high, i), dims, preferred_element_type=jnp.float32)
    once = lax.dot_general(top, matrix(low, i), dims, preferred_element_type=jnp.float32)
    return twice[:count] + (twice[count:] + once)


def to_pairs(v):
    root = float(np.sqrt(0.5))
    s = [v[b] + v[b + 4] for b in range(4)]
    d = [v[b] - v[b + 4] for b in range(4)]
    even, odd = s[0] + s[2], s[1] + s[3]
    near, far = root * (d[1] - d[3]), root * (d[1] + d[3])
    pairs = (
        (even + odd, even - odd),
        (d[0] + near, far + d[2]),
        (s[0] - s[2], s[1] - s[3]),
        (d[0] - near, far - d[2]),
    )
    return [jnp.concatenate(pair, axis=1) for pair in pairs]


def to_modes(pairs, high, low):
    return [product(pair, high, low, i) for i, pair in enumerate(pairs)]


def to_cells(h, high, low, product=product):
    root = float(np.sqrt(0.5))
    width = high.shape[1]
    pairs = [product(h[i], high, low, i) for i in range(4)]
    (a0, a4), (a1, b1), (a2, b2), (a3, b3) = [(pair[:, :width], pair[:, width:]) for pair in pairs]
    e, g = a0 + a4, a0 - a4
    p, m, q, n = a1 + a3, a1 - a3, b1 + b3, b1 - b3
    ep, em, gp, gm = e + a2, e - a2, g + b2, g - b2
    up, down = root * (m + q), root * (q - m)
    return [ep + p, gp + up, em + n, gm + down, ep - p, gp - up, em - n, gm - down]


def write_symbols(out_ref, length):
    residues, _, group, width = out_ref.shape
    device = 0
    for axis in AXES:
        device = device * lax.axis_size(axis) + lax.axis_index(axis)
    groups = width // group
    residue = jnp.int32(0)
    for i, q in enumerate(RESIDUES):
        residue = jnp.where(device // groups == i, q, residue)
    within = lax.rem(device, groups) * group
    sublane = lax.broadcasted_iota(jnp.int32, (group, width), 0)
    lane = lax.broadcasted_iota(jnp.int32, (group, width), 1)

    def half_sines(modes):
        return jnp.sin(jnp.pi / length * modes.astype(jnp.float32)) ** 2

    column_sines = half_sines(residue + RADIX * (within + sublane))
    for q in range(residues):
        stiffness = 4.0 * (half_sines(q + RADIX * lane) + column_sines)
        fine = 1.0 / (1.0 + decay_rate + spread_rate * stiffness)
        power, forcing_symbol = fine, fine
        for _ in range(M - 1):
            power = power * fine
            forcing_symbol = forcing_symbol + power
        out_ref[q, 0] = power
        out_ref[q, 1] = forcing_symbol
        out_ref[q, 2] = 1.0 / (1.0 + M * decay_rate + M * spread_rate * stiffness)


def columns_forward(guess_ref, start_ref, source_ref, high_ref, low_ref, out_ref, symbols_ref, field, high, low, copied):
    last = lax.axis_size("z") * lax.axis_size("y") - 1
    place = lax.axis_index("z") * lax.axis_size("y") + lax.axis_index("y")

    def fetch(ref):
        pltpu.make_async_copy(ref, field, copied.at[0]).start()

    @pl.when(place < last - 1)
    def _():
        fetch(guess_ref.at[0])

    @pl.when(place == last - 1)
    def _():
        fetch(start_ref)

    @pl.when(place == last)
    def _():
        fetch(source_ref)

    matrices = [
        pltpu.make_async_copy(high_ref, high, copied.at[1]),
        pltpu.make_async_copy(low_ref, low, copied.at[2]),
    ]
    for copy in matrices:
        copy.start()
    write_symbols(symbols_ref, field.shape[1])
    pltpu.make_async_copy(start_ref, field, copied.at[0]).wait()

    width = field.shape[1] // RADIX
    pairs = to_pairs([field[:, b * width : (b + 1) * width] for b in range(RADIX)])
    for copy in matrices:
        copy.wait()
    for i in range(4):
        out_ref[2 * width * i : 2 * width * (i + 1), :] = product_across(pairs[i], high, low, i)


def rows_and_time(in_ref, symbols_ref, high_ref, low_ref, high_across_ref, low_across_ref, out_ref):
    group, width = in_ref.shape[len(AXES) :]
    sizes = dict(zip(AXES, in_ref.shape))
    times, blocks = sizes["z"] * sizes["y"], sizes["x"] * sizes["core"]
    length = blocks * width
    rows = times * group

    def of_block(b):
        place = {"x": b // sizes["core"], "core": b % sizes["core"]}
        return tuple(place.get(axis, slice(None)) for axis in AXES)

    v = [in_ref[of_block(b)].reshape(rows, width) for b in range(blocks)]
    h = to_modes(to_pairs(v), high_ref, low_ref)

    outs = []
    for i in range(4):
        first, second = RESIDUES[2 * i], RESIDUES[2 * i + 1]
        power, forcing_symbol, coarse = (
            jnp.concatenate([symbols_ref[first, j], symbols_ref[second, j]], axis=1) for j in range(3)
        )
        scale = 1.0 / (length * length)
        scaled_power = scale * power
        part = [h[i][t * group : (t + 1) * group] for t in range(times)]
        forcing = scale * forcing_symbol * part[times - 1]
        relaxed = scaled_power * part[times - 2] + forcing
        state = relaxed
        states = [state]
        gap = power - coarse
        for j in range(1, times):
            state = coarse * state + (gap * relaxed + forcing)
            states.append(state)
            if j < times - 1:
                relaxed = scaled_power * part[j - 1] + forcing
        outs.append(jnp.concatenate(states, axis=0))

    cells = to_cells(outs, high_across_ref, low_across_ref)
    for b in range(blocks):
        place = of_block(b)
        out_ref[place] = cells[b].reshape(sizes["z"], sizes["y"], group, width)


def columns_inverse(in_ref, high_ref, low_ref, out_ref):
    width = in_ref.shape[1]
    h = [in_ref[2 * width * i : 2 * width * (i + 1), :] for i in range(4)]
    cells = to_cells(h, high_ref, low_ref, product_down)
    for b in range(RADIX):
        out_ref[0, :, b * width : (b + 1) * width] = cells[b]


def on_chip(count):
    return [pl.BlockSpec(memory_space=pltpu.VMEM)] * count


def off_chip(count):
    return [pl.BlockSpec(memory_space=pltpu.HBM)] * count


def body(initial_guess, start_field, source_field):
    rows, length = start_field.shape
    devices = lax.axis_size(AXES)
    tiles = tuple(lax.axis_size(axis) for axis in AXES)
    group = length // devices
    matrices = kernel_matrices(length)
    high, low = (jnp.asarray(part) for part in matrices)
    high_across, low_across = (jnp.asarray(np.swapaxes(part, 1, 2)) for part in matrices)

    symbols = (max(RESIDUES) + 1, 3, group, length // RADIX)
    spectra, symbols = pl.pallas_call(
        columns_forward,
        out_shape=[jax.ShapeDtypeStruct(shape, jnp.float32) for shape in ((length, rows), symbols)],
        in_specs=off_chip(5),
        out_specs=on_chip(2),
        scratch_shapes=[
            pltpu.VMEM((rows, length), jnp.float32),
            pltpu.VMEM(high.shape, high.dtype),
            pltpu.VMEM(low.shape, low.dtype),
            pltpu.SemaphoreType.DMA((3,)),
        ],
        compiler_params=LIMIT,
        name="columns_forward",
    )(*(pltpu.with_memory_space_constraint(x, pltpu.HBM) for x in (initial_guess, start_field, source_field, high_across, low_across)))

    spectra = spectra.reshape(devices, group, rows)
    spectra = lax.all_to_all(spectra, AXES, split_axis=0, concat_axis=0, tiled=True)
    states = pl.pallas_call(
        rows_and_time,
        out_shape=jax.ShapeDtypeStruct(tiles + (group, rows), jnp.float32),
        in_specs=on_chip(6),
        out_specs=on_chip(1)[0],
        compiler_params=LIMIT,
        name="rows_and_time",
    )(spectra.reshape(tiles + (group, rows)), symbols, high, low, high_across, low_across)

    states = states.reshape(devices, group, rows)
    states = lax.all_to_all(states, AXES, split_axis=0, concat_axis=0, tiled=True)
    return pl.pallas_call(
        columns_inverse,
        out_shape=jax.ShapeDtypeStruct((1, rows, length), jnp.float32),
        in_specs=on_chip(3),
        out_specs=on_chip(1)[0],
        compiler_params=LIMIT,
        name="columns_inverse",
    )(states.reshape(length, rows), high_across, low_across)


def solution(mesh):
    chips = mesh.shape["space"] // 2
    finer = Mesh(mesh.devices.reshape(4, -1, chips, 2), TM + SPACE)
    in_specs = (P(TM, SPACE, None), P(SPACE, None), P(SPACE, None))
    out_specs = P(TM, SPACE, None)
    return jax.shard_map(body, mesh=finer, in_specs=in_specs, out_specs=out_specs, check_vma=False)
```

```python
import jax
import jax.numpy as jnp
import ml_dtypes
import numpy as np
from jax import lax
from jax.experimental import pallas as pl
from jax.experimental.pallas import tpu as pltpu
from jax.sharding import Mesh
from jax.sharding import PartitionSpec as P

M = 16
RADIX = 8
RESIDUES = (0, 4, 1, 1, 2, 2, 3, 3)
AXES = ("core", "z", "x", "y")
TM, SPACE = ("z", "y"), ("x", "core")
LIMIT = pltpu.CompilerParams(vmem_limit_bytes=8 * 1024 * 1024)

decay_rate = 0.0005
spread_rate = 0.01


def kernel_matrices(length):
    width = length // RADIX
    cells = np.arange(width)

    def cas(residue, sign):
        modes = residue + RADIX * np.arange(width)
        angles = 2.0 * np.pi / length * (cells[:, None] * modes[None, :] % length)
        return np.cos(angles) + sign * np.sin(angles)

    blocks = [cas(0, 1), cas(4, 1)] + [cas(q, sign) for q in (1, 2, 3) for sign in (1, -1)]
    full = np.stack(blocks).astype(np.float32)
    high = full.astype(ml_dtypes.bfloat16)
    low = (full - high.astype(np.float32)).astype(ml_dtypes.bfloat16)
    return high, low


def matrix(blocks, i):
    one, other = blocks[2 * i], blocks[2 * i + 1]
    if i == 0:
        zero = jnp.zeros_like(one)
        rows = ((one, zero), (zero, other))
    else:
        rows = ((one, other), (other, -one))
    return jnp.concatenate([jnp.concatenate(row, axis=1) for row in rows], axis=0)


def split(value):
    high = value.astype(jnp.bfloat16)
    low = (value - high.astype(jnp.float32)).astype(jnp.bfloat16)
    return jnp.concatenate([high, low], axis=0)


def product(value, high, low, i):
    count, modes = value.shape
    parts = split(value)

    def times(left, upper, lower):
        twice = jnp.dot(left, upper, preferred_element_type=jnp.float32)
        once = jnp.dot(left[:count], lower, preferred_element_type=jnp.float32)
        return twice[:count] + (twice[count:] + once)

    if i == 0:
        half = modes // 2
        sides = (times(parts[:, j * half : (j + 1) * half], high[j], low[j]) for j in range(2))
        return jnp.concatenate(list(sides), axis=1)
    return times(parts, matrix(high, i), matrix(low, i))


def product_across(value, high, low, i):
    count, modes = value.shape
    matrices = jnp.concatenate([matrix(high, i), matrix(low, i)], axis=0)
    dims = (((1,), (1,)), ((), ()))
    both = lax.dot_general(matrices, split(value), dims, preferred_element_type=jnp.float32)
    return both[:modes, :count] + (both[:modes, count:] + both[modes:, :count])


def product_down(value, high, low, i):
    count = value.shape[1]
    top = value.astype(jnp.bfloat16)
    rest = (value - top.astype(jnp.float32)).astype(jnp.bfloat16)
    parts = jnp.concatenate([top, rest], axis=1)
    dims = (((0,), (0,)), ((), ()))
    twice = lax.dot_general(parts, matrix(high, i), dims, preferred_element_type=jnp.float32)
    once = lax.dot_general(top, matrix(low, i), dims, preferred_element_type=jnp.float32)
    return twice[:count] + (twice[count:] + once)


def to_pairs(v):
    root = float(np.sqrt(0.5))
    s = [v[b] + v[b + 4] for b in range(4)]
    d = [v[b] - v[b + 4] for b in range(4)]
    even, odd = s[0] + s[2], s[1] + s[3]
    near, far = root * (d[1] - d[3]), root * (d[1] + d[3])
    pairs = (
        (even + odd, even - odd),
        (d[0] + near, far + d[2]),
        (s[0] - s[2], s[1] - s[3]),
        (d[0] - near, far - d[2]),
    )
    return [jnp.concatenate(pair, axis=1) for pair in pairs]


def to_modes(pairs, high, low):
    return [product(pair, high, low, i) for i, pair in enumerate(pairs)]


def to_cells(h, high, low, product=product):
    root = float(np.sqrt(0.5))
    width = high.shape[1]
    pairs = [product(h[i], high, low, i) for i in range(4)]
    (a0, a4), (a1, b1), (a2, b2), (a3, b3) = [(pair[:, :width], pair[:, width:]) for pair in pairs]
    e, g = a0 + a4, a0 - a4
    p, m, q, n = a1 + a3, a1 - a3, b1 + b3, b1 - b3
    ep, em, gp, gm = e + a2, e - a2, g + b2, g - b2
    up, down = root * (m + q), root * (q - m)
    return [ep + p, gp + up, em + n, gm + down, ep - p, gp - up, em - n, gm - down]


def write_symbols(out_ref, length):
    residues, _, group, width = out_ref.shape
    device = 0
    for axis in AXES:
        device = device * lax.axis_size(axis) + lax.axis_index(axis)
    groups = width // group
    residue = jnp.int32(0)
    for i, q in enumerate(RESIDUES):
        residue = jnp.where(device // groups == i, q, residue)
    within = lax.rem(device, groups) * group
    sublane = lax.broadcasted_iota(jnp.int32, (group, width), 0)
    lane = lax.broadcasted_iota(jnp.int32, (group, width), 1)

    def half_sines(modes):
        return jnp.sin(jnp.pi / length * modes.astype(jnp.float32)) ** 2

    column_sines = half_sines(residue + RADIX * (within + sublane))
    for q in range(residues):
        stiffness = 4.0 * (half_sines(q + RADIX * lane) + column_sines)
        fine = 1.0 / (1.0 + decay_rate + spread_rate * stiffness)
        power, forcing_symbol = fine, fine
        for _ in range(M - 1):
            power = power * fine
            forcing_symbol = forcing_symbol + power
        out_ref[q, 0] = power
        out_ref[q, 1] = forcing_symbol
        out_ref[q, 2] = 1.0 / (1.0 + M * decay_rate + M * spread_rate * stiffness)


def columns_forward(guess_ref, start_ref, source_ref, high_ref, low_ref, out_ref, symbols_ref, field, high, low, copied):
    last = lax.axis_size("z") * lax.axis_size("y") - 1
    place = lax.axis_index("z") * lax.axis_size("y") + lax.axis_index("y")

    def fetch(ref):
        pltpu.make_async_copy(ref, field, copied.at[0]).start()

    @pl.when(place < last - 1)
    def _():
        fetch(guess_ref.at[0])

    @pl.when(place == last - 1)
    def _():
        fetch(start_ref)

    @pl.when(place == last)
    def _():
        fetch(source_ref)

    matrices = [
        pltpu.make_async_copy(high_ref, high, copied.at[1]),
        pltpu.make_async_copy(low_ref, low, copied.at[2]),
    ]
    for copy in matrices:
        copy.start()
    write_symbols(symbols_ref, field.shape[1])
    pltpu.make_async_copy(start_ref, field, copied.at[0]).wait()

    width = field.shape[1] // RADIX
    pairs = to_pairs([field[:, b * width : (b + 1) * width] for b in range(RADIX)])
    for copy in matrices:
        copy.wait()
    for i in range(4):
        out_ref[2 * width * i : 2 * width * (i + 1), :] = product_across(pairs[i], high, low, i)


def rows_and_time(in_ref, symbols_ref, high_ref, low_ref, high_across_ref, low_across_ref, out_ref):
    group, width = in_ref.shape[len(AXES) :]
    sizes = dict(zip(AXES, in_ref.shape))
    times, blocks = sizes["z"] * sizes["y"], sizes["x"] * sizes["core"]
    length = blocks * width
    rows = times * group

    def of_block(b):
        place = {"x": b // sizes["core"], "core": b % sizes["core"]}
        return tuple(place.get(axis, slice(None)) for axis in AXES)

    v = [in_ref[of_block(b)].reshape(rows, width) for b in range(blocks)]
    h = to_modes(to_pairs(v), high_ref, low_ref)

    outs = []
    for i in range(4):
        first, second = RESIDUES[2 * i], RESIDUES[2 * i + 1]
        power, forcing_symbol, coarse = (
            jnp.concatenate([symbols_ref[first, j], symbols_ref[second, j]], axis=1) for j in range(3)
        )
        scale = 1.0 / (length * length)
        scaled_power = scale * power
        part = [h[i][t * group : (t + 1) * group] for t in range(times)]
        forcing = scale * forcing_symbol * part[times - 1]
        relaxed = scaled_power * part[times - 2] + forcing
        state = relaxed
        states = [state]
        gap = power - coarse
        for j in range(1, times):
            state = coarse * state + (gap * relaxed + forcing)
            states.append(state)
            if j < times - 1:
                relaxed = scaled_power * part[j - 1] + forcing
        outs.append(jnp.concatenate(states, axis=0))

    cells = to_cells(outs, high_across_ref, low_across_ref)
    for b in range(blocks):
        place = of_block(b)
        out_ref[place] = cells[b].reshape(sizes["z"], sizes["y"], group, width)


def columns_inverse(in_ref, high_ref, low_ref, out_ref):
    width = in_ref.shape[1]
    h = [in_ref[2 * width * i : 2 * width * (i + 1), :] for i in range(4)]
    cells = to_cells(h, high_ref, low_ref, product_down)
    for b in range(RADIX):
        out_ref[0, :, b * width : (b + 1) * width] = cells[b]


def on_chip(count):
    return [pl.BlockSpec(memory_space=pltpu.VMEM)] * count


def off_chip(count):
    return [pl.BlockSpec(memory_space=pltpu.HBM)] * count


def body(initial_guess, start_field, source_field):
    rows, length = start_field.shape
    devices = lax.axis_size(AXES)
    tiles = tuple(lax.axis_size(axis) for axis in AXES)
    group = length // devices
    matrices = kernel_matrices(length)
    high, low = (jnp.asarray(part) for part in matrices)
    high_across, low_across = (jnp.asarray(np.swapaxes(part, 1, 2)) for part in matrices)

    symbols = (max(RESIDUES) + 1, 3, group, length // RADIX)
    spectra, symbols = pl.pallas_call(
        columns_forward,
        out_shape=[jax.ShapeDtypeStruct(shape, jnp.float32) for shape in ((length, rows), symbols)],
        in_specs=off_chip(5),
        out_specs=on_chip(2),
        scratch_shapes=[
            pltpu.VMEM((rows, length), jnp.float32),
            pltpu.VMEM(high.shape, high.dtype),
            pltpu.VMEM(low.shape, low.dtype),
            pltpu.SemaphoreType.DMA((3,)),
        ],
        compiler_params=LIMIT,
        name="columns_forward",
    )(*(pltpu.with_memory_space_constraint(x, pltpu.HBM) for x in (initial_guess, start_field, source_field, high_across, low_across)))

    spectra = spectra.reshape(devices, group, rows)
    spectra = lax.all_to_all(spectra, AXES, split_axis=0, concat_axis=0, tiled=True)
    states = pl.pallas_call(
        rows_and_time,
        out_shape=jax.ShapeDtypeStruct(tiles + (group, rows), jnp.float32),
        in_specs=on_chip(6),
        out_specs=on_chip(1)[0],
        compiler_params=LIMIT,
        name="rows_and_time",
    )(spectra.reshape(tiles + (group, rows)), symbols, high, low, high_across, low_across)

    states = states.reshape(devices, group, rows)
    states = lax.all_to_all(states, AXES, split_axis=0, concat_axis=0, tiled=True)
    return pl.pallas_call(
        columns_inverse,
        out_shape=jax.ShapeDtypeStruct((1, rows, length), jnp.float32),
        in_specs=on_chip(3),
        out_specs=on_chip(1)[0],
        compiler_params=LIMIT,
        name="columns_inverse",
    )(states.reshape(length, rows), high_across, low_across)


def solution(mesh):
    chips = mesh.shape["space"] // 2
    finer = Mesh(mesh.devices.reshape(4, -1, chips, 2), TM + SPACE)
    in_specs = (P(TM, SPACE, None), P(SPACE, None), P(SPACE, None))
    out_specs = P(TM, SPACE, None)
    return jax.shard_map(body, mesh=finer, in_specs=in_specs, out_specs=out_specs, check_vma=False)
```

```python
import jax
import jax.numpy as jnp
import ml_dtypes
import numpy as np
from jax import lax
from jax.experimental import pallas as pl
from jax.experimental.pallas import tpu as pltpu
from jax.sharding import Mesh
from jax.sharding import PartitionSpec as P

M = 16
RADIX = 8
RESIDUES = (0, 4, 1, 1, 2, 2, 3, 3)
AXES = ("core", "z", "x", "y")
TM, SPACE = ("z", "y"), ("x", "core")
LIMIT = pltpu.CompilerParams(vmem_limit_bytes=8 * 1024 * 1024)

decay_rate = 0.0005
spread_rate = 0.01


def kernel_matrices(length):
    width = length // RADIX
    cells = np.arange(width)

    def cas(residue, sign):
        modes = residue + RADIX * np.arange(width)
        angles = 2.0 * np.pi / length * (cells[:, None] * modes[None, :] % length)
        return np.cos(angles) + sign * np.sin(angles)

    blocks = [cas(0, 1), cas(4, 1)] + [cas(q, sign) for q in (1, 2, 3) for sign in (1, -1)]
    full = np.stack(blocks).astype(np.float32)
    high = full.astype(ml_dtypes.bfloat16)
    low = (full - high.astype(np.float32)).astype(ml_dtypes.bfloat16)
    return high, low


def matrix(blocks, i):
    one, other = blocks[2 * i], blocks[2 * i + 1]
    if i == 0:
        zero = jnp.zeros_like(one)
        rows = ((one, zero), (zero, other))
    else:
        rows = ((one, other), (other, -one))
    return jnp.concatenate([jnp.concatenate(row, axis=1) for row in rows], axis=0)


def split(value):
    high = value.astype(jnp.bfloat16)
    low = (value - high.astype(jnp.float32)).astype(jnp.bfloat16)
    return jnp.concatenate([high, low], axis=0)


def product(value, high, low, i):
    count, modes = value.shape
    parts = split(value)

    def times(left, upper, lower):
        twice = jnp.dot(left, upper, preferred_element_type=jnp.float32)
        once = jnp.dot(left[:count], lower, preferred_element_type=jnp.float32)
        return twice[:count] + (twice[count:] + once)

    if i == 0:
        half = modes // 2
        sides = (times(parts[:, j * half : (j + 1) * half], high[j], low[j]) for j in range(2))
        return jnp.concatenate(list(sides), axis=1)
    return times(parts, matrix(high, i), matrix(low, i))


def product_across(value, high, low, i):
    count, modes = value.shape
    parts = split(value)
    dims = (((1,), (1,)), ((), ()))

    def times(upper, lower, right):
        modes = upper.shape[0]
        matrices = jnp.concatenate([upper, lower], axis=0)
        both = lax.dot_general(matrices, right, dims, preferred_element_type=jnp.float32)
        return both[:modes, :count] + (both[:modes, count:] + both[modes:, :count])

    if i == 0:
        half = modes // 2
        sides = (times(high[j], low[j], parts[:, j * half : (j + 1) * half]) for j in range(2))
        return jnp.concatenate(list(sides), axis=0)
    return times(matrix(high, i), matrix(low, i), parts)


def product_down(value, high, low, i):
    count = value.shape[1]
    top = value.astype(jnp.bfloat16)
    rest = (value - top.astype(jnp.float32)).astype(jnp.bfloat16)
    parts = jnp.concatenate([top, rest], axis=1)
    dims = (((0,), (0,)), ((), ()))
    twice = lax.dot_general(parts, matrix(high, i), dims, preferred_element_type=jnp.float32)
    once = lax.dot_general(top, matrix(low, i), dims, preferred_element_type=jnp.float32)
    return twice[:count] + (twice[count:] + once)


def to_pairs(v):
    root = float(np.sqrt(0.5))
    s = [v[b] + v[b + 4] for b in range(4)]
    d = [v[b] - v[b + 4] for b in range(4)]
    even, odd = s[0] + s[2], s[1] + s[3]
    near, far = root * (d[1] - d[3]), root * (d[1] + d[3])
    pairs = (
        (even + odd, even - odd),
        (d[0] + near, far + d[2]),
        (s[0] - s[2], s[1] - s[3]),
        (d[0] - near, far - d[2]),
    )
    return [jnp.concatenate(pair, axis=1) for pair in pairs]


def to_modes(pairs, high, low):
    return [product(pair, high, low, i) for i, pair in enumerate(pairs)]


def to_cells(h, high, low, product=product):
    root = float(np.sqrt(0.5))
    width = high.shape[1]
    pairs = [product(h[i], high, low, i) for i in range(4)]
    (a0, a4), (a1, b1), (a2, b2), (a3, b3) = [(pair[:, :width], pair[:, width:]) for pair in pairs]
    e, g = a0 + a4, a0 - a4
    p, m, q, n = a1 + a3, a1 - a3, b1 + b3, b1 - b3
    ep, em, gp, gm = e + a2, e - a2, g + b2, g - b2
    up, down = root * (m + q), root * (q - m)
    return [ep + p, gp + up, em + n, gm + down, ep - p, gp - up, em - n, gm - down]


def write_symbols(out_ref, length):
    residues, _, group, width = out_ref.shape
    device = 0
    for axis in AXES:
        device = device * lax.axis_size(axis) + lax.axis_index(axis)
    groups = width // group
    residue = jnp.int32(0)
    for i, q in enumerate(RESIDUES):
        residue = jnp.where(device // groups == i, q, residue)
    within = lax.rem(device, groups) * group
    sublane = lax.broadcasted_iota(jnp.int32, (group, width), 0)
    lane = lax.broadcasted_iota(jnp.int32, (group, width), 1)

    def half_sines(modes):
        return jnp.sin(jnp.pi / length * modes.astype(jnp.float32)) ** 2

    column_sines = half_sines(residue + RADIX * (within + sublane))
    for q in range(residues):
        stiffness = 4.0 * (half_sines(q + RADIX * lane) + column_sines)
        fine = 1.0 / (1.0 + decay_rate + spread_rate * stiffness)
        power, forcing_symbol = fine, fine
        for _ in range(M - 1):
            power = power * fine
            forcing_symbol = forcing_symbol + power
        out_ref[q, 0] = power
        out_ref[q, 1] = forcing_symbol
        out_ref[q, 2] = 1.0 / (1.0 + M * decay_rate + M * spread_rate * stiffness)


def columns_forward(guess_ref, start_ref, source_ref, high_ref, low_ref, out_ref, symbols_ref, field, high, low, copied):
    last = lax.axis_size("z") * lax.axis_size("y") - 1
    place = lax.axis_index("z") * lax.axis_size("y") + lax.axis_index("y")

    def fetch(ref):
        pltpu.make_async_copy(ref, field, copied.at[0]).start()

    @pl.when(place < last - 1)
    def _():
        fetch(guess_ref.at[0])

    @pl.when(place == last - 1)
    def _():
        fetch(start_ref)

    @pl.when(place == last)
    def _():
        fetch(source_ref)

    matrices = [
        pltpu.make_async_copy(high_ref, high, copied.at[1]),
        pltpu.make_async_copy(low_ref, low, copied.at[2]),
    ]
    for copy in matrices:
        copy.start()
    write_symbols(symbols_ref, field.shape[1])
    pltpu.make_async_copy(start_ref, field, copied.at[0]).wait()

    width = field.shape[1] // RADIX
    pairs = to_pairs([field[:, b * width : (b + 1) * width] for b in range(RADIX)])
    for copy in matrices:
        copy.wait()
    for i in range(4):
        out_ref[2 * width * i : 2 * width * (i + 1), :] = product_across(pairs[i], high, low, i)


def rows_and_time(in_ref, symbols_ref, high_ref, low_ref, high_across_ref, low_across_ref, out_ref):
    group, width = in_ref.shape[len(AXES) :]
    sizes = dict(zip(AXES, in_ref.shape))
    times, blocks = sizes["z"] * sizes["y"], sizes["x"] * sizes["core"]
    length = blocks * width
    rows = times * group

    def of_block(b):
        place = {"x": b // sizes["core"], "core": b % sizes["core"]}
        return tuple(place.get(axis, slice(None)) for axis in AXES)

    v = [in_ref[of_block(b)].reshape(rows, width) for b in range(blocks)]
    h = to_modes(to_pairs(v), high_ref, low_ref)

    outs = []
    for i in range(4):
        first, second = RESIDUES[2 * i], RESIDUES[2 * i + 1]
        power, forcing_symbol, coarse = (
            jnp.concatenate([symbols_ref[first, j], symbols_ref[second, j]], axis=1) for j in range(3)
        )
        scale = 1.0 / (length * length)
        scaled_power = scale * power
        part = [h[i][t * group : (t + 1) * group] for t in range(times)]
        forcing = scale * forcing_symbol * part[times - 1]
        relaxed = scaled_power * part[times - 2] + forcing
        state = relaxed
        states = [state]
        gap = power - coarse
        for j in range(1, times):
            state = coarse * state + (gap * relaxed + forcing)
            states.append(state)
            if j < times - 1:
                relaxed = scaled_power * part[j - 1] + forcing
        outs.append(jnp.concatenate(states, axis=0))

    cells = to_cells(outs, high_across_ref, low_across_ref)
    for b in range(blocks):
        place = of_block(b)
        out_ref[place] = cells[b].reshape(sizes["z"], sizes["y"], group, width)


def columns_inverse(in_ref, high_ref, low_ref, out_ref):
    width = in_ref.shape[1]
    h = [in_ref[2 * width * i : 2 * width * (i + 1), :] for i in range(4)]
    cells = to_cells(h, high_ref, low_ref, product_down)
    for b in range(RADIX):
        out_ref[0, :, b * width : (b + 1) * width] = cells[b]


def on_chip(count):
    return [pl.BlockSpec(memory_space=pltpu.VMEM)] * count


def off_chip(count):
    return [pl.BlockSpec(memory_space=pltpu.HBM)] * count


def body(initial_guess, start_field, source_field):
    rows, length = start_field.shape
    devices = lax.axis_size(AXES)
    tiles = tuple(lax.axis_size(axis) for axis in AXES)
    group = length // devices
    matrices = kernel_matrices(length)
    high, low = (jnp.asarray(part) for part in matrices)
    high_across, low_across = (jnp.asarray(np.swapaxes(part, 1, 2)) for part in matrices)

    symbols = (max(RESIDUES) + 1, 3, group, length // RADIX)
    spectra, symbols = pl.pallas_call(
        columns_forward,
        out_shape=[jax.ShapeDtypeStruct(shape, jnp.float32) for shape in ((length, rows), symbols)],
        in_specs=off_chip(5),
        out_specs=on_chip(2),
        scratch_shapes=[
            pltpu.VMEM((rows, length), jnp.float32),
            pltpu.VMEM(high.shape, high.dtype),
            pltpu.VMEM(low.shape, low.dtype),
            pltpu.SemaphoreType.DMA((3,)),
        ],
        compiler_params=LIMIT,
        name="columns_forward",
    )(*(pltpu.with_memory_space_constraint(x, pltpu.HBM) for x in (initial_guess, start_field, source_field, high_across, low_across)))

    spectra = spectra.reshape(devices, group, rows)
    spectra = lax.all_to_all(spectra, AXES, split_axis=0, concat_axis=0, tiled=True)
    states = pl.pallas_call(
        rows_and_time,
        out_shape=jax.ShapeDtypeStruct(tiles + (group, rows), jnp.float32),
        in_specs=on_chip(6),
        out_specs=on_chip(1)[0],
        compiler_params=LIMIT,
        name="rows_and_time",
    )(spectra.reshape(tiles + (group, rows)), symbols, high, low, high_across, low_across)

    states = states.reshape(devices, group, rows)
    states = lax.all_to_all(states, AXES, split_axis=0, concat_axis=0, tiled=True)
    return pl.pallas_call(
        columns_inverse,
        out_shape=jax.ShapeDtypeStruct((1, rows, length), jnp.float32),
        in_specs=on_chip(3),
        out_specs=on_chip(1)[0],
        compiler_params=LIMIT,
        name="columns_inverse",
    )(states.reshape(length, rows), high_across, low_across)


def solution(mesh):
    chips = mesh.shape["space"] // 2
    finer = Mesh(mesh.devices.reshape(4, -1, chips, 2), TM + SPACE)
    in_specs = (P(TM, SPACE, None), P(SPACE, None), P(SPACE, None))
    out_specs = P(TM, SPACE, None)
    return jax.shard_map(body, mesh=finer, in_specs=in_specs, out_specs=out_specs, check_vma=False)
```
